64 devices in a mesh: rep: 4 (over x, y), dp: 16 (over z, core).
Axes of the slice: x: 2, y: 2, z: 8, core: 2. Of those that a mesh axis runs over, the one named last changes fastest.
The devices are a block of a 4x4x8 slice.
Arguments:
- g_w_gate: bfloat16 [64, 2, 640, 2176], P(('rep', 'dp')), parts along dimension 0
- g_w_up: bfloat16 [64, 2, 640, 2176], P(('rep', 'dp')), parts along dimension 0
- g_w_down: bfloat16 [64, 2, 2176, 640], P(('rep', 'dp')), parts along dimension 0
- w_gate: bfloat16 [2, 640, 2176], replicated
- w_up: bfloat16 [2, 640, 2176], replicated
- w_down: bfloat16 [2, 2176, 640], replicated
- m_w_gate: float32 [2, 640, 2176], P(None, 'dp')
- m_w_up: float32 [2, 640, 2176], P(None, 'dp')
- m_w_down: float32 [2, 2176, 640], P(None, 'dp')
- v_w_gate: float32 [2, 640, 2176], P(None, 'dp')
- v_w_up: float32 [2, 640, 2176], P(None, 'dp')
- v_w_down: float32 [2, 2176, 640], P(None, 'dp')
Outputs:
- output 1: bfloat16 [8, 640, 2176], P('rep'), parts along dimension 0
- output 2: bfloat16 [8, 640, 2176], P('rep'), parts along dimension 0
- output 3: bfloat16 [8, 2176, 640], P('rep'), parts along dimension 0
- output 4: float32 [8, 640, 2176], P('rep', 'dp'), parts along dimension 0
- output 5: float32 [8, 640, 2176], P('rep', 'dp'), parts along dimension 0
- output 6: float32 [8, 2176, 640], P('rep', 'dp'), parts along dimension 0
- output 7: float32 [8, 640, 2176], P('rep', 'dp'), parts along dimension 0
- output 8: float32 [8, 640, 2176], P('rep', 'dp'), parts along dimension 0
- output 9: float32 [8, 2176, 640], P('rep', 'dp'), parts along dimension 0
There are 4 independent parts. The reference program is written for one: setup_inputs(seed, part) draws one part's arguments, and reference() takes and returns one part's arrays. A program takes and returns all parts, laid end to end along the dimension named above; an argument that names none is the same for every part.
All inputs are finite; a program needn't handle non-finite values.
Results may differ from the reference program's by a relative error of at most 0.022.
Values are sent between devices in bfloat16 or wider.
A program may use at most 768 MiB of HBM per device.

```python
import jax
import jax.numpy as jnp
from jax import lax

DEVICES = 16
D = 640
FF = 2176
LAYERS = 2
NAMES = ("w_gate", "w_up", "w_down")
SHAPES = {"w_gate": (LAYERS, D, FF), "w_up": (LAYERS, D, FF), "w_down": (LAYERS, FF, D)}


def setup_inputs(seed: int = 0, part: int = 0) -> dict:
    kz, *keys = jax.random.split(jax.random.key(seed), 1 + 5 * len(NAMES))
    loud = 2.0 ** jax.random.uniform(kz, (), jnp.float32, -1.0, 1.0)
    drawn = {}
    for name, key, both in zip(NAMES, keys[:3], keys[3:6], strict=True):
        own = jax.random.normal(jax.random.fold_in(key, part), (DEVICES, *SHAPES[name]), jnp.float32)
        shared = jax.random.normal(jax.random.fold_in(both, part), SHAPES[name], jnp.float32)
        drawn["g_" + name] = (loud * (0.7 * shared / DEVICES + 0.7 * own * DEVICES**-0.5)).astype(jnp.bfloat16)
    for name, key in zip(NAMES, keys[6:9], strict=True):
        drawn[name] = (jax.random.normal(key, SHAPES[name], jnp.float32) * SHAPES[name][1] ** -0.5).astype(jnp.bfloat16)
    for name, key in zip(NAMES, keys[9:12], strict=True):
        drawn["m_" + name] = loud * 0.5 * jax.random.normal(key, SHAPES[name], jnp.float32)
    for name, key in zip(NAMES, keys[12:15], strict=True):
        drawn["v_" + name] = loud * loud * jax.random.uniform(key, SHAPES[name], jnp.float32, 0.5, 1.5)
    return drawn


def adamw(w, m, v, g):
    m = 0.9 * m + 0.1 * g
    v = 0.95 * v + 0.05 * g * g
    step = m * lax.rsqrt(v + 1e-8) + 0.1 * w
    return (w - 0.02 * step).astype(jnp.bfloat16), m, v


def clipped(gradients, sum_of_squares, count):
    factor = jnp.minimum(1.0, 0.5 * lax.rsqrt(sum_of_squares / count + 1e-30))
    return [g * factor for g in gradients]


def reference(g_w_gate, g_w_up, g_w_down, w_gate, w_up, w_down, m_w_gate, m_w_up, m_w_down, v_w_gate, v_w_up, v_w_down):
    def total(terms):
        return lax.scan(lambda so_far, term: (so_far + term.astype(jnp.float32), None), jnp.zeros(terms.shape[1:], jnp.float32), terms)[0]

    gradients = [total(terms).astype(jnp.bfloat16).astype(jnp.float32) for terms in (g_w_gate, g_w_up, g_w_down)]
    gradients = clipped(gradients, sum(jnp.sum(g * g) for g in gradients), sum(g.size for g in gradients))
    new = [
        adamw(w.astype(jnp.float32), m, v, g)
        for w, m, v, g in zip((w_gate, w_up, w_down), (m_w_gate, m_w_up, m_w_down), (v_w_gate, v_w_up, v_w_down), gradients, strict=True)
    ]
    return tuple(one[which] for which in range(3) for one in new)
```

```python
import functools

import jax
import jax.numpy as jnp
from jax import lax
from jax.experimental import pallas as pl
from jax.experimental.pallas import tpu as pltpu
from jax.sharding import PartitionSpec as P

CORES = 2
ROWS = 8
WEIGHTS = 3
LANES = 128


def rows_of(ref, lead, start, count):
    return ref.at[(*lead, pl.ds(pl.multiple_of(start, ROWS), count))]


def step_kernel(n, count, *refs):
    take = iter(refs)
    three = lambda: [next(take) for _ in range(WEIGHTS)]
    grads, old, m_in, v_in = three(), three(), three(), three()
    whole, m, v = three(), three(), three()
    mine, theirs, ring = three(), three(), three()
    squares, parts = next(take), next(take)
    (load_sem, swap_send, swap_recv, ring_send, ring_recv, gather_send, gather_recv, give_send, give_recv, state_sem, part_send, part_recv) = take

    chips = n // CORES
    me = lax.axis_index("dp")
    chip, core = me // CORES, lax.rem(me, CORES)
    other = chip * CORES + 1 - core
    ahead = lax.rem(chip + 1, chips) * CORES + core
    behind = lax.rem(chip + chips - 1, chips) * CORES + core
    toward = (ahead, behind)

    def to(device):
        return dict(device_id={"dp": device}, device_id_type=pl.DeviceIdType.MESH)

    def chip_at(way, back):
        return lax.rem(chip + chips - back, chips) if way == 0 else lax.rem(chip + back, chips)

    def height(k):
        return m[k].shape[1]

    pieces = [(k, way) for k in range(WEIGHTS) for way in (0, 1)]

    def load(k, way, s):
        at = (chip_at(way, s + 1) * CORES + core) * height(k)
        return pltpu.make_async_copy(rows_of(grads[k], (0, way), at, height(k)), mine[k].at[s, way], load_sem.at[k, way, s])

    def swap(k, way, s):
        at = (chip_at(way, s + 1) * CORES + 1 - core) * height(k)
        return pltpu.make_async_remote_copy(
            rows_of(grads[k], (0, way), at, height(k)), theirs[k].at[s, way], swap_send.at[k, way, s], swap_recv.at[k, way, s], **to(other)
        )

    def hop(k, way, s):
        return pltpu.make_async_remote_copy(
            mine[k].at[s, way], ring[k].at[s, way], ring_send.at[k, way, s], ring_recv.at[k, way, s], **to(toward[way])
        )

    def place(k, way, back, at_core):
        return rows_of(whole[k], (way,), (chip_at(way, back) * CORES + at_core) * height(k), height(k))

    def pass_on(k, way, s):
        block = place(k, way, s, core)
        return pltpu.make_async_remote_copy(block, block, gather_send.at[k, way, s], gather_recv.at[k, way, s], **to(toward[way]))

    def give(k, way, s):
        block = place(k, way, s, core)
        return pltpu.make_async_remote_copy(block, block, give_send.at[k, way, s], give_recv.at[k, way, s], **to(other))

    def arrived(k, way, s):
        block = place(k, way, s + 1, core)
        return pltpu.make_async_remote_copy(block, block, gather_send.at[k, way, s], gather_recv.at[k, way, s], **to(toward[way]))

    def given(k, way, s):
        block = place(k, way, s, 1 - core)
        return pltpu.make_async_remote_copy(block, block, give_send.at[k, way, s], give_recv.at[k, way, s], **to(other))

    def state(k):
        for way in (0, 1):
            yield pltpu.make_async_copy(
                rows_of(old[k], (way,), me * height(k), height(k)), place(k, way, 0, core), state_sem.at[k, way]
            )
        yield pltpu.make_async_copy(m_in[k], m[k], state_sem.at[k, 2])
        yield pltpu.make_async_copy(v_in[k], v[k], state_sem.at[k, 3])

    def part_to(d):
        peer = lax.rem(me + d, n)
        return pltpu.make_async_remote_copy(parts.at[0], parts.at[d], part_send.at[d], part_recv.at[d], **to(peer))

    for k, way in pieces:
        load(k, way, 0).start()

    barrier = pltpu.get_barrier_semaphore()
    for device in (other, ahead, behind):
        pl.semaphore_signal(barrier, inc=1, **to(device))
    pl.semaphore_wait(barrier, 3)

    for k, way in pieces:
        swap(k, way, 0).start()

    @pl.loop(1, chips)
    def _(s):
        for k, way in pieces:
            swap(k, way, s).start()
            load(k, way, s).start()

    for k in range(WEIGHTS):
        for copy in state(k):
            copy.start()

    def add(k, way, s, with_ring):
        @pl.loop(0, height(k) // ROWS)
        def _(i):
            r = pl.ds(pl.multiple_of(i * ROWS, ROWS), ROWS)
            total = mine[k][s, way, r, :].astype(jnp.float32) + theirs[k][s, way, r, :].astype(jnp.float32)
            if with_ring:
                total += ring[k][s - 1, way, r, :].astype(jnp.float32)
            mine[k][s, way, r, :] = total.astype(jnp.bfloat16)

    for k, way in pieces:
        load(k, way, 0).wait()
        swap(k, way, 0).wait_recv()
        add(k, way, 0, False)
        hop(k, way, 0).start()

    @pl.loop(1, chips - 1)
    def _(s):
        for k, way in pieces:
            load(k, way, s).wait()
            swap(k, way, s).wait_recv()
            hop(k, way, s - 1).wait_recv()
            add(k, way, s, True)
            hop(k, way, s).start()

    last = chips - 1
    squares[...] = jnp.zeros_like(squares)

    def fold(x):
        return sum(x[:, c : c + LANES] for c in range(0, x.shape[1], LANES))

    for k, way in pieces:
        load(k, way, last).wait()
        swap(k, way, last).wait_recv()
        hop(k, way, last - 1).wait_recv()

        @pl.loop(0, height(k) // ROWS)
        def _(i):
            r = pl.ds(pl.multiple_of(i * ROWS, ROWS), ROWS)
            total = mine[k][last, way, r, :].astype(jnp.float32) + theirs[k][last, way, r, :].astype(jnp.float32)
            total += ring[k][last - 1, way, r, :].astype(jnp.float32)
            g = total.astype(jnp.bfloat16)
            mine[k][last, way, r, :] = g
            g = g.astype(jnp.float32)
            squares[...] += fold(g * g)

    parts[0] = squares[...]
    for d in range(1, n):
        part_to(d).start()
    for k in range(WEIGHTS):
        for copy in state(k):
            copy.wait()
    everything = squares[...]
    for d in range(1, n):
        part_to(d).wait_recv()
        everything = everything + parts[d]
    factor = jnp.minimum(1.0, 0.5 * lax.rsqrt(jnp.full((1, LANES), jnp.sum(everything), jnp.float32) / count + 1e-30))[0, 0]

    for k, way in pieces:
        start = pl.multiple_of(me * height(k), ROWS)

        @pl.loop(0, height(k) // ROWS)
        def _(i):
            r = pl.ds(pl.multiple_of(i * ROWS, ROWS), ROWS)
            at = pl.ds(pl.multiple_of(start + i * ROWS, ROWS), ROWS)
            g = mine[k][last, way, r, :].astype(jnp.float32) * factor
            w = whole[k][way, at, :].astype(jnp.float32)
            new_m = 0.9 * m[k][way, r, :] + 0.1 * g
            new_v = 0.95 * v[k][way, r, :] + 0.05 * g * g
            m[k][way, r, :] = new_m
            v[k][way, r, :] = new_v
            change = new_m * lax.rsqrt(new_v + 1e-8) + 0.1 * w
            whole[k][way, at, :] = (w - 0.02 * change).astype(jnp.bfloat16)

        pass_on(k, way, 0).start()
        give(k, way, 0).start()

    @pl.loop(0, chips - 2)
    def _(s):
        for k, way in pieces:
            arrived(k, way, s).wait_recv()
            pass_on(k, way, s + 1).start()
            give(k, way, s + 1).start()

    for k, way in pieces:
        arrived(k, way, last - 1).wait_recv()
        give(k, way, last).start()

    for d in range(1, n):
        part_to(d).wait_send()

    @pl.loop(0, chips)
    def _(s):
        for k, way in pieces:
            swap(k, way, s).wait_send()
            given(k, way, s).wait_recv()

    @pl.loop(0, chips - 1)
    def _(s):
        for k, way in pieces:
            hop(k, way, s).wait_send()
            pass_on(k, way, s).wait_send()

    @pl.loop(0, chips)
    def _(s):
        for k, way in pieces:
            give(k, way, s).wait_send()


def solution(mesh):
    n = mesh.shape["dp"]
    chips = n // CORES

    def step(*arrays):
        terms, weights, m, v = (arrays[i : i + 3] for i in (0, 3, 6, 9))
        count = float(sum(w.size for w in weights))
        whole = [pltpu.VMEM(w.shape, w.dtype) for w in weights]
        moments = [pltpu.VMEM(a.shape, a.dtype) for a in (*m, *v)]
        blocks = [a.shape for a in m]
        dma = pltpu.SemaphoreType.DMA
        two = (WEIGHTS, 2)
        return pl.pallas_call(
            functools.partial(step_kernel, n, count),
            out_shape=(*whole, *moments),
            in_specs=[pl.BlockSpec(memory_space=pl.ANY)] * 12,
            out_specs=[pl.BlockSpec(memory_space=pltpu.VMEM)] * 9,
            scratch_shapes=[
                *(pltpu.VMEM((chips, *b), jnp.bfloat16) for b in blocks),
                *(pltpu.VMEM((chips, *b), jnp.bfloat16) for b in blocks),
                *(pltpu.VMEM((chips - 1, *b), jnp.bfloat16) for b in blocks),
                pltpu.VMEM((ROWS, LANES), jnp.float32),
                pltpu.VMEM((n, ROWS, LANES), jnp.float32),
                dma((*two, chips)),
                dma((*two, chips)),
                dma((*two, chips)),
                dma((*two, chips - 1)),
                dma((*two, chips - 1)),
                dma((*two, chips - 1)),
                dma((*two, chips - 1)),
                dma((*two, chips)),
                dma((*two, chips)),
                dma((WEIGHTS, 4)),
                dma((n,)),
                dma((n,)),
            ],
            compiler_params=pltpu.CompilerParams(collective_id=0, has_side_effects=True, vmem_limit_bytes=34 * 2**20),
        )(*arrays)

    all_of, cut = P(None, None, None), P(None, "dp", None)
    return jax.shard_map(
        step,
        mesh=mesh,
        in_specs=(P(("rep", "dp"), None, None, None),) * 3 + (all_of,) * 3 + (cut,) * 6,
        out_specs=(P("rep", None, None),) * 3 + (P("rep", "dp", None),) * 6,
        check_vma=False,
    )
```

```python
import functools

import jax
import jax.numpy as jnp
from jax import lax
from jax.experimental import pallas as pl
from jax.experimental.pallas import tpu as pltpu
from jax.sharding import PartitionSpec as P

CORES = 2
ROWS = 8
WEIGHTS = 3
LANES = 128


def rows_of(ref, lead, start, count):
    return ref.at[(*lead, pl.ds(pl.multiple_of(start, ROWS), count))]


def step_kernel(n, count, *refs):
    take = iter(refs)
    three = lambda: [next(take) for _ in range(WEIGHTS)]
    grads, old, m_in, v_in = three(), three(), three(), three()
    whole, m, v = three(), three(), three()
    mine, theirs, ring = three(), three(), three()
    squares, parts = next(take), next(take)
    (load_sem, swap_send, swap_recv, ring_send, ring_recv, gather_send, gather_recv, give_send, give_recv, state_sem, part_send, part_recv) = take

    chips = n // CORES
    me = lax.axis_index("dp")
    chip, core = me // CORES, lax.rem(me, CORES)
    other = chip * CORES + 1 - core
    ahead = lax.rem(chip + 1, chips) * CORES + core
    behind = lax.rem(chip + chips - 1, chips) * CORES + core
    toward = (ahead, behind)

    def to(device):
        return dict(device_id={"dp": device}, device_id_type=pl.DeviceIdType.MESH)

    def chip_at(way, back):
        return lax.rem(chip + chips - back, chips) if way == 0 else lax.rem(chip + back, chips)

    def height(k):
        return m[k].shape[1]

    pieces = [(k, way) for k in range(WEIGHTS) for way in (0, 1)]

    def load(k, way, s):
        at = (chip_at(way, s + 1) * CORES + core) * height(k)
        return pltpu.make_async_copy(rows_of(grads[k], (0, way), at, height(k)), mine[k].at[s, way], load_sem.at[k, way, s])

    def swap(k, way, s):
        at = (chip_at(way, s + 1) * CORES + 1 - core) * height(k)
        return pltpu.make_async_remote_copy(
            rows_of(grads[k], (0, way), at, height(k)), theirs[k].at[s, way], swap_send.at[k, way, s], swap_recv.at[k, way, s], **to(other)
        )

    def hop(k, way, s):
        return pltpu.make_async_remote_copy(
            mine[k].at[s, way], ring[k].at[s, way], ring_send.at[k, way, s], ring_recv.at[k, way, s], **to(toward[way])
        )

    def place(k, way, back, at_core):
        return rows_of(whole[k], (way,), (chip_at(way, back) * CORES + at_core) * height(k), height(k))

    def pass_on(k, way, s):
        block = place(k, way, s, core)
        return pltpu.make_async_remote_copy(block, block, gather_send.at[k, way, s], gather_recv.at[k, way, s], **to(toward[way]))

    def give(k, way, s):
        block = place(k, way, s, core)
        return pltpu.make_async_remote_copy(block, block, give_send.at[k, way, s], give_recv.at[k, way, s], **to(other))

    def arrived(k, way, s):
        block = place(k, way, s + 1, core)
        return pltpu.make_async_remote_copy(block, block, gather_send.at[k, way, s], gather_recv.at[k, way, s], **to(toward[way]))

    def given(k, way, s):
        block = place(k, way, s, 1 - core)
        return pltpu.make_async_remote_copy(block, block, give_send.at[k, way, s], give_recv.at[k, way, s], **to(other))

    def state(k):
        for way in (0, 1):
            yield pltpu.make_async_copy(
                rows_of(old[k], (way,), me * height(k), height(k)), place(k, way, 0, core), state_sem.at[k, way]
            )
        yield pltpu.make_async_copy(m_in[k], m[k], state_sem.at[k, 2])
        yield pltpu.make_async_copy(v_in[k], v[k], state_sem.at[k, 3])

    def part_to(d):
        peer = lax.rem(me + d, n)
        return pltpu.make_async_remote_copy(parts.at[0], parts.at[d], part_send.at[d], part_recv.at[d], **to(peer))

    for k, way in pieces:
        load(k, way, 0).start()

    barrier = pltpu.get_barrier_semaphore()
    for device in (other, ahead, behind):
        pl.semaphore_signal(barrier, inc=1, **to(device))
    pl.semaphore_wait(barrier, 3)

    for k, way in pieces:
        swap(k, way, 0).start()

    @pl.loop(1, chips)
    def _(s):
        for k, way in pieces:
            swap(k, way, s).start()
            load(k, way, s).start()

    for k in range(WEIGHTS):
        for copy in state(k):
            copy.start()

    def add(k, way, s, with_ring):
        @pl.loop(0, height(k) // ROWS)
        def _(i):
            r = pl.ds(pl.multiple_of(i * ROWS, ROWS), ROWS)
            total = mine[k][s, way, r, :].astype(jnp.float32) + theirs[k][s, way, r, :].astype(jnp.float32)
            if with_ring:
                total += ring[k][s - 1, way, r, :].astype(jnp.float32)
            mine[k][s, way, r, :] = total.astype(jnp.bfloat16)

    for k, way in pieces:
        load(k, way, 0).wait()
        swap(k, way, 0).wait_recv()
        add(k, way, 0, False)
        hop(k, way, 0).start()

    @pl.loop(1, chips - 1)
    def _(s):
        for k, way in pieces:
            load(k, way, s).wait()
            swap(k, way, s).wait_recv()
            hop(k, way, s - 1).wait_recv()
            add(k, way, s, True)
            hop(k, way, s).start()

    last = chips - 1
    squares[...] = jnp.zeros_like(squares)

    def fold(x):
        return sum(x[:, c : c + LANES] for c in range(0, x.shape[1], LANES))

    for k, way in pieces:
        load(k, way, last).wait()
        swap(k, way, last).wait_recv()
        hop(k, way, last - 1).wait_recv()

        @pl.loop(0, height(k) // ROWS)
        def _(i):
            r = pl.ds(pl.multiple_of(i * ROWS, ROWS), ROWS)
            total = mine[k][last, way, r, :].astype(jnp.float32) + theirs[k][last, way, r, :].astype(jnp.float32)
            total += ring[k][last - 1, way, r, :].astype(jnp.float32)
            g = total.astype(jnp.bfloat16)
            mine[k][last, way, r, :] = g
            g = g.astype(jnp.float32)
            squares[...] += fold(g * g)

    parts[0] = squares[...]
    for d in range(1, n):
        part_to(d).start()
    for k in range(WEIGHTS):
        for copy in state(k):
            copy.wait()
    everything = squares[...]
    for d in range(1, n):
        part_to(d).wait_recv()
        everything = everything + parts[d]
    factor = jnp.minimum(1.0, 0.5 * lax.rsqrt(jnp.full((1, LANES), jnp.sum(everything), jnp.float32) / count + 1e-30))[0, 0]

    for k, way in pieces:
        start = pl.multiple_of(me * height(k), ROWS)

        @pl.loop(0, height(k) // ROWS)
        def _(i):
            r = pl.ds(pl.multiple_of(i * ROWS, ROWS), ROWS)
            at = pl.ds(pl.multiple_of(start + i * ROWS, ROWS), ROWS)
            g = mine[k][last, way, r, :].astype(jnp.float32) * factor
            w = whole[k][way, at, :].astype(jnp.float32)
            new_m = 0.9 * m[k][way, r, :] + 0.1 * g
            new_v = 0.95 * v[k][way, r, :] + 0.05 * g * g
            m[k][way, r, :] = new_m
            v[k][way, r, :] = new_v
            change = new_m * lax.rsqrt(new_v + 1e-8) + 0.1 * w
            whole[k][way, at, :] = (w - 0.02 * change).astype(jnp.bfloat16)

        pass_on(k, way, 0).start()
        give(k, way, 0).start()

    @pl.loop(0, chips - 2)
    def _(s):
        for k, way in pieces:
            arrived(k, way, s).wait_recv()
            pass_on(k, way, s + 1).start()
            give(k, way, s + 1).start()

    for k, way in pieces:
        arrived(k, way, last - 1).wait_recv()
        give(k, way, last).start()

    for d in range(1, n):
        part_to(d).wait_send()

    @pl.loop(0, chips)
    def _(s):
        for k, way in pieces:
            swap(k, way, s).wait_send()
            given(k, way, s).wait_recv()

    @pl.loop(0, chips - 1)
    def _(s):
        for k, way in pieces:
            hop(k, way, s).wait_send()
            pass_on(k, way, s).wait_send()

    @pl.loop(0, chips)
    def _(s):
        for k, way in pieces:
            give(k, way, s).wait_send()


def store_kernel(*refs):
    half = len(refs) // 2
    results, outs, sems = refs[:half], refs[half:-1], refs[-1]
    copies = [
        pltpu.make_async_copy(a.at[layer], b.at[layer], sems.at[i, layer])
        for i, (a, b) in enumerate(zip(results, outs, strict=True))
        for layer in range(a.shape[0])
    ]
    for copy in copies:
        copy.start()
    for copy in copies:
        copy.wait()


def solution(mesh):
    n = mesh.shape["dp"]
    chips = n // CORES

    def step(*arrays):
        terms, weights, m, v = (arrays[i : i + 3] for i in (0, 3, 6, 9))
        count = float(sum(w.size for w in weights))
        whole = [pltpu.VMEM(w.shape, w.dtype) for w in weights]
        moments = [pltpu.VMEM(a.shape, a.dtype) for a in (*m, *v)]
        blocks = [a.shape for a in m]
        dma = pltpu.SemaphoreType.DMA
        two = (WEIGHTS, 2)
        results = pl.pallas_call(
            functools.partial(step_kernel, n, count),
            out_shape=(*whole, *moments),
            in_specs=[pl.BlockSpec(memory_space=pl.ANY)] * 12,
            out_specs=[pl.BlockSpec(memory_space=pltpu.VMEM)] * 9,
            scratch_shapes=[
                *(pltpu.VMEM((chips, *b), jnp.bfloat16) for b in blocks),
                *(pltpu.VMEM((chips, *b), jnp.bfloat16) for b in blocks),
                *(pltpu.VMEM((chips - 1, *b), jnp.bfloat16) for b in blocks),
                pltpu.VMEM((ROWS, LANES), jnp.float32),
                pltpu.VMEM((n, ROWS, LANES), jnp.float32),
                dma((*two, chips)),
                dma((*two, chips)),
                dma((*two, chips)),
                dma((*two, chips - 1)),
                dma((*two, chips - 1)),
                dma((*two, chips - 1)),
                dma((*two, chips - 1)),
                dma((*two, chips)),
                dma((*two, chips)),
                dma((WEIGHTS, 4)),
                dma((n,)),
                dma((n,)),
            ],
            compiler_params=pltpu.CompilerParams(collective_id=0, has_side_effects=True, vmem_limit_bytes=34 * 2**20),
        )(*arrays)
        return pl.pallas_call(
            store_kernel,
            out_shape=[jax.ShapeDtypeStruct(a.shape, a.dtype) for a in results],
            in_specs=[pl.BlockSpec(memory_space=pltpu.VMEM)] * 9,
            out_specs=[pl.BlockSpec(memory_space=pl.ANY)] * 9,
            scratch_shapes=[dma((9, 2))],
            compiler_params=pltpu.CompilerParams(vmem_limit_bytes=2**20),
        )(*results)

    all_of, cut = P(None, None, None), P(None, "dp", None)
    return jax.shard_map(
        step,
        mesh=mesh,
        in_specs=(P(("rep", "dp"), None, None, None),) * 3 + (all_of,) * 3 + (cut,) * 6,
        out_specs=(P("rep", None, None),) * 3 + (P("rep", "dp", None),) * 6,
        check_vma=False,
    )
```

```python
import functools

import jax
import jax.numpy as jnp
from jax import lax
from jax.experimental import pallas as pl
from jax.experimental.pallas import tpu as pltpu
from jax.sharding import PartitionSpec as P

CORES = 2
ROWS = 8
WEIGHTS = 3
LANES = 128


def rows_of(ref, lead, start, count):
    return ref.at[(*lead, pl.ds(pl.multiple_of(start, ROWS), count))]


def step_kernel(n, count, *refs):
    take = iter(refs)
    three = lambda: [next(take) for _ in range(WEIGHTS)]
    grads, old, m_in, v_in = three(), three(), three(), three()
    whole, m, v = three(), three(), three()
    mine, theirs, ring = three(), three(), three()
    squares, parts = next(take), next(take)
    load_sem, swap_send, swap_recv, ring_send, hop_recv, gather_send, give_send, give_recv, state_sem, part_sem = take

    chips = n // CORES
    me = lax.axis_index("dp")
    chip, core = me // CORES, lax.rem(me, CORES)
    other = chip * CORES + 1 - core
    ahead = lax.rem(chip + 1, chips) * CORES + core
    behind = lax.rem(chip + chips - 1, chips) * CORES + core
    toward = (ahead, behind)

    def to(device):
        return dict(device_id={"dp": device}, device_id_type=pl.DeviceIdType.MESH)

    def chip_at(way, back):
        return lax.rem(chip + chips - back, chips) if way == 0 else lax.rem(chip + back, chips)

    def height(k):
        return m[k].shape[1]

    pieces = [(k, way) for k in range(WEIGHTS) for way in (0, 1)]

    def first(s):
        return 0 if isinstance(s, int) and s == 0 else 1

    def load(k, way, s):
        at = (chip_at(way, s + 1) * CORES + core) * height(k)
        return pltpu.make_async_copy(rows_of(grads[k], (0, way), at, height(k)), mine[k].at[s, way], load_sem.at[k, first(s)])

    def swap(k, way, s, slot):
        at = (chip_at(way, s + 1) * CORES + 1 - core) * height(k)
        return pltpu.make_async_remote_copy(
            rows_of(grads[k], (0, way), at, height(k)), theirs[k].at[s, way], swap_send.at[k], swap_recv.at[k, slot], **to(other)
        )

    def hop(k, way, s):
        return pltpu.make_async_remote_copy(
            mine[k].at[s, way], ring[k].at[s, way], ring_send.at[k], hop_recv.at[k, way, s], **to(toward[way])
        )

    def place(k, way, back, at_core):
        return rows_of(whole[k], (way,), (chip_at(way, back) * CORES + at_core) * height(k), height(k))

    def pass_on(k, way, s):
        block = place(k, way, s, core)
        return pltpu.make_async_remote_copy(block, block, gather_send.at[k], hop_recv.at[k, way, s], **to(toward[way]))

    def give(k, way, s):
        block = place(k, way, s, core)
        return pltpu.make_async_remote_copy(block, block, give_send.at[k], give_recv.at[k], **to(other))

    def await_bytes(ref, sem):
        pltpu.make_async_copy(ref, ref, sem).wait()

    def await_hop(k, way, s):
        await_bytes(ring[k].at[s, way], hop_recv.at[k, way, s])

    def start_state(k):
        for way in (0, 1):
            pltpu.make_async_copy(rows_of(old[k], (way,), me * height(k), height(k)), place(k, way, 0, core), state_sem.at[k, 0]).start()
        pltpu.make_async_copy(m_in[k], m[k], state_sem.at[k, 1]).start()
        pltpu.make_async_copy(v_in[k], v[k], state_sem.at[k, 2]).start()

    def await_state(k):
        await_bytes(mine[k].at[0], state_sem.at[k, 0])
        await_bytes(m[k], state_sem.at[k, 1])
        await_bytes(v[k], state_sem.at[k, 2])

    def part_to(d):
        return pltpu.make_async_remote_copy(parts.at[0], parts.at[d], part_sem.at[0], part_sem.at[1], **to(lax.rem(me + d, n)))

    barrier = pltpu.get_barrier_semaphore()
    for device in (other, ahead, behind):
        pl.semaphore_signal(barrier, inc=1, **to(device))
    pl.semaphore_wait(barrier, 3)

    for k, way in pieces:
        swap(k, way, 0, way).start()
        load(k, way, 0).start()
    for k, way in pieces:
        swap(k, way, 1, 2).start()
        load(k, way, 1).start()

    @pl.loop(2, chips)
    def _(s):
        for k, way in pieces:
            swap(k, way, s, 3).start()
            load(k, way, s).start()

    for k in range(WEIGHTS):
        start_state(k)

    def add(k, way, s, with_ring):
        @pl.loop(0, height(k) // ROWS)
        def _(i):
            r = pl.ds(pl.multiple_of(i * ROWS, ROWS), ROWS)
            total = mine[k][s, way, r, :].astype(jnp.float32) + theirs[k][s, way, r, :].astype(jnp.float32)
            if with_ring:
                total += ring[k][s - 1, way, r, :].astype(jnp.float32)
            mine[k][s, way, r, :] = total.astype(jnp.bfloat16)

    for k, way in pieces:
        if way == 0:
            await_bytes(mine[k].at[0], load_sem.at[k, 0])
        await_bytes(theirs[k].at[0, way], swap_recv.at[k, way])
        add(k, way, 0, False)
        hop(k, way, 0).start()

    for k, way in pieces:
        if way == 0:
            await_bytes(mine[k].at[pl.ds(1, chips - 1)], load_sem.at[k, 1])
            await_bytes(theirs[k].at[1], swap_recv.at[k, 2])
        await_hop(k, way, 0)
        add(k, way, 1, True)
        hop(k, way, 1).start()

    for k in range(WEIGHTS):
        await_bytes(theirs[k].at[pl.ds(2, chips - 2)], swap_recv.at[k, 3])

    @pl.loop(2, chips - 1)
    def _(s):
        for k, way in pieces:
            await_hop(k, way, s - 1)
            add(k, way, s, True)
            hop(k, way, s).start()

    for k in range(WEIGHTS):
        await_state(k)

    last = chips - 1
    squares[...] = jnp.zeros_like(squares)

    def fold(x):
        return sum(x[:, c : c + LANES] for c in range(0, x.shape[1], LANES))

    for k, way in pieces:
        await_hop(k, way, last - 1)

        @pl.loop(0, height(k) // ROWS)
        def _(i):
            r = pl.ds(pl.multiple_of(i * ROWS, ROWS), ROWS)
            total = mine[k][last, way, r, :].astype(jnp.float32) + theirs[k][last, way, r, :].astype(jnp.float32)
            total += ring[k][last - 1, way, r, :].astype(jnp.float32)
            g = total.astype(jnp.bfloat16)
            mine[k][last, way, r, :] = g
            g = g.astype(jnp.float32)
            squares[...] += fold(g * g)

    parts[0] = jnp.sum(squares[...], axis=0, keepdims=True)
    for d in sorted(range(1, n), key=lambda d: -min(d, n - d)):
        part_to(d).start()
    await_bytes(parts.at[pl.ds(1, n - 1)], part_sem.at[1])
    everything = sum(parts[d] for d in range(n))
    factor = jnp.minimum(1.0, 0.5 * lax.rsqrt(jnp.sum(everything, keepdims=True) / count + 1e-30))[0, 0]

    for k, way in pieces:
        start = pl.multiple_of(me * height(k), ROWS)

        @pl.loop(0, height(k) // ROWS)
        def _(i):
            r = pl.ds(pl.multiple_of(i * ROWS, ROWS), ROWS)
            at = pl.ds(pl.multiple_of(start + i * ROWS, ROWS), ROWS)
            g = mine[k][last, way, r, :].astype(jnp.float32) * factor
            w = whole[k][way, at, :].astype(jnp.float32)
            new_m = 0.9 * m[k][way, r, :] + 0.1 * g
            new_v = 0.95 * v[k][way, r, :] + 0.05 * g * g
            m[k][way, r, :] = new_m
            v[k][way, r, :] = new_v
            change = new_m * lax.rsqrt(new_v + 1e-8) + 0.1 * w
            whole[k][way, at, :] = (w - 0.02 * change).astype(jnp.bfloat16)

        pass_on(k, way, 0).start()
        give(k, way, 0).start()

    @pl.loop(0, chips - 2)
    def _(s):
        for k, way in pieces:
            await_hop(k, way, s)
            pass_on(k, way, s + 1).start()
            give(k, way, s + 1).start()

    for k, way in pieces:
        await_hop(k, way, last - 1)
        give(k, way, last).start()

    await_bytes(parts.at[pl.ds(1, n - 1)], part_sem.at[0])
    for k in range(WEIGHTS):
        everywhere = whole[k].at[:, pl.ds(0, chips * height(k))]
        await_bytes(mine[k], swap_send.at[k])
        await_bytes(mine[k].at[pl.ds(0, last)], ring_send.at[k])
        await_bytes(mine[k].at[pl.ds(0, last)], gather_send.at[k])
        await_bytes(everywhere, give_recv.at[k])
        await_bytes(everywhere, give_send.at[k])


def store_kernel(*refs):
    half = len(refs) // 2
    results, outs, sems = refs[:half], refs[half:-1], refs[-1]
    copies = [
        pltpu.make_async_copy(a.at[layer], b.at[layer], sems.at[i, layer])
        for i, (a, b) in enumerate(zip(results, outs, strict=True))
        for layer in range(a.shape[0])
    ]
    for copy in copies:
        copy.start()
    for copy in copies:
        copy.wait()


def solution(mesh):
    n = mesh.shape["dp"]
    chips = n // CORES

    def step(*arrays):
        terms, weights, m, v = (arrays[i : i + 3] for i in (0, 3, 6, 9))
        count = float(sum(w.size for w in weights))
        whole = [pltpu.VMEM(w.shape, w.dtype) for w in weights]
        moments = [pltpu.VMEM(a.shape, a.dtype) for a in (*m, *v)]
        blocks = [a.shape for a in m]
        dma = pltpu.SemaphoreType.DMA
        results = pl.pallas_call(
            functools.partial(step_kernel, n, count),
            out_shape=(*whole, *moments),
            in_specs=[pl.BlockSpec(memory_space=pl.ANY)] * 12,
            out_specs=[pl.BlockSpec(memory_space=pltpu.VMEM)] * 9,
            scratch_shapes=[
                *(pltpu.VMEM((chips, *b), jnp.bfloat16) for b in blocks),
                *(pltpu.VMEM((chips, *b), jnp.bfloat16) for b in blocks),
                *(pltpu.VMEM((chips - 1, *b), jnp.bfloat16) for b in blocks),
                pltpu.VMEM((ROWS, LANES), jnp.float32),
                pltpu.VMEM((n, 1, LANES), jnp.float32),
                dma((WEIGHTS, 2)),
                dma((WEIGHTS,)),
                dma((WEIGHTS, 4)),
                dma((WEIGHTS,)),
                dma((WEIGHTS, 2, chips - 1)),
                dma((WEIGHTS,)),
                dma((WEIGHTS,)),
                dma((WEIGHTS,)),
                dma((WEIGHTS, 3)),
                dma((2,)),
            ],
            compiler_params=pltpu.CompilerParams(collective_id=0, has_side_effects=True, vmem_limit_bytes=34 * 2**20),
        )(*arrays)
        return pl.pallas_call(
            store_kernel,
            out_shape=[jax.ShapeDtypeStruct(a.shape, a.dtype) for a in results],
            in_specs=[pl.BlockSpec(memory_space=pltpu.VMEM)] * 9,
            out_specs=[pl.BlockSpec(memory_space=pl.ANY)] * 9,
            scratch_shapes=[dma((9, 2))],
            compiler_params=pltpu.CompilerParams(vmem_limit_bytes=2**20),
        )(*results)

    all_of, cut = P(None, None, None), P(None, "dp", None)
    return jax.shard_map(
        step,
        mesh=mesh,
        in_specs=(P(("rep", "dp"), None, None, None),) * 3 + (all_of,) * 3 + (cut,) * 6,
        out_specs=(P("rep", None, None),) * 3 + (P("rep", "dp", None),) * 6,
        check_vma=False,
    )
```
